256 devices in a mesh: grp: 8 (over y, core), chan: 32 (over z, x).
Axes of the slice: x: 4, y: 4, z: 8, core: 2. Of those that a mesh axis runs over, the one named last changes fastest.
Arguments:
- fibre_records: bfloat16 [2048, 256, 1536], P(('grp', 'chan')), may hold values from -6 to 6
- station_records: bfloat16 [1024, 256, 1536], P('chan'), may hold values from -6 to 6
- band_mask: int32 [8, 256], replicated, may hold values 0 or 1
- station_valid: int32 [1024], P('chan'), may hold values 0 or 1
- segment_keep: int32 [256], replicated, may hold values 0 or 1
Outputs:
- cross_spectra: float32 [2, 8, 2048, 1024], P(None, None, ('grp', 'chan'))
The draws below stay inside these ranges and needn't reach their ends.
All inputs are finite; a program needn't handle non-finite values. No bound on the sum of `station_valid` on one device may be relied on, other than what follows from the above.
Results may differ from the reference program's by a relative error of at most 0.0072.
Values may be sent and summed in bfloat16 or wider, within the bound.
No kernel may reach another device: no remote copies, remote signals or barrier semaphores. Data moves between devices by JAX's collectives and lax.ppermute only.
A program may use at most 128 MiB of HBM per device.

```python
import math
import jax
import jax.numpy as jnp
from jax import lax

SEG = 256
SAMPLES = 1536
NFREQ = 8
FIRST_BIN = 24
STA = 1024
KCH = 256
CHANNELS = 2048
N_GRP = 8


def with_ends(array, rng, least, top_value):
    longest = array.shape.index(max(array.shape))
    spots = []
    for shift in (0, 1):
        where = [jax.random.randint(jax.random.fold_in(rng, axis), (), 0, length) for axis, length in enumerate(array.shape)]
        where[longest] = (where[longest] + shift) % array.shape[longest]
        spots.append(tuple(where))
    return array.at[spots[0]].set(least).at[spots[1]].set(top_value)


def shard_levels(key, shape, cuts, low, top_value):
    level, own = 1.0, jax.random.fold_in(key, 6)
    for dim, shards_of in cuts:
        steps = jnp.exp(jax.random.uniform(jax.random.fold_in(own, dim), (shards_of,), jnp.float32, low / len(cuts), top_value / len(cuts)))
        level = level * jnp.repeat(steps, shape[dim] // shards_of).reshape([-1 if axis == dim else 1 for axis in range(len(shape))])
    return level


def bell_draw(key, shape, spread, reach, cuts=(), kind=jnp.bfloat16):
    array = jax.random.normal(key, shape, jnp.float32) * spread
    if len(cuts) > 0:
        array = shard_levels(key, shape, cuts, -0.22, 0.18) * array
    return jnp.clip(array, min=-reach, max=reach).astype(kind)


def setup_inputs(seed: int = 0) -> dict:
    key_list = jax.random.split(jax.random.key(seed), 6)
    return {
        "fibre_records": bell_draw(key_list[0], (CHANNELS, SEG, SAMPLES), 1.0, 6.0, ((0, 256),)),
        "station_records": bell_draw(key_list[1], (STA, SEG, SAMPLES), 1.0, 6.0, ((0, 32),)),
        "band_mask": with_ends((jax.random.randint(key_list[2], (NFREQ, KCH), 0, 8) < 5).astype(jnp.int32), jax.random.fold_in(key_list[2], 1), 0, 1),
        "station_valid": with_ends((jax.random.randint(key_list[3], (STA,), 0, 8) < 7).astype(jnp.int32), jax.random.fold_in(key_list[3], 1), 0, 1),
        "segment_keep": with_ends((jax.random.randint(key_list[4], (SEG,), 0, 4) < 3).astype(jnp.int32), jax.random.fold_in(key_list[4], 1), 0, 1),
    }


def time_table():
    sample_index = jnp.arange(SAMPLES, dtype=jnp.int32)
    bin_index = FIRST_BIN + jnp.arange(NFREQ, dtype=jnp.int32)
    phase = sample_index[:, None] * bin_index[None, :] % SAMPLES
    angle = phase.astype(jnp.float32) * (2.0 * math.pi / SAMPLES)
    return jnp.concatenate([jnp.cos(angle), -jnp.sin(angle)], axis=1).astype(jnp.bfloat16)

def wave_tables(width):
    index = jnp.arange(width, dtype=jnp.int32)
    phase = index[:, None] * index[None, :] % width
    angle = phase.astype(jnp.float32) * (2.0 * math.pi / width)
    return (jnp.cos(angle).astype(jnp.bfloat16), jnp.sin(angle).astype(jnp.bfloat16))

def matmul(left, right):
    return jnp.dot(left, right, preferred_element_type=jnp.float32)

def wavenumber_filter(spectra, cosines, sines, weights):
    width, count = (spectra.shape[0], spectra.shape[1])
    real_part = spectra[:, :, :NFREQ].reshape(width, count * NFREQ)
    imag_part = spectra[:, :, NFREQ:].reshape(width, count * NFREQ)
    fwd_real = matmul(cosines, real_part) + matmul(sines, imag_part)
    fwd_imag = matmul(cosines, imag_part) - matmul(sines, real_part)
    fwd_real = (fwd_real.reshape(width, count, NFREQ) * weights[:, None, :]).astype(jnp.bfloat16).reshape(width, count * NFREQ)
    fwd_imag = (fwd_imag.reshape(width, count, NFREQ) * weights[:, None, :]).astype(jnp.bfloat16).reshape(width, count * NFREQ)
    back_real = (matmul(cosines, fwd_real) - matmul(sines, fwd_imag)) / width
    back_imag = (matmul(sines, fwd_real) + matmul(cosines, fwd_imag)) / width
    joined = jnp.concatenate([back_real.reshape(width, count, NFREQ), back_imag.reshape(width, count, NFREQ)], axis=2)
    return joined.astype(jnp.bfloat16)

def scale_rows(spectra, totals, valid):
    factor = lax.rsqrt(totals / (2 * SEG * NFREQ) + 1e-06) * valid.astype(jnp.float32)
    return (spectra * factor[:, None, None]).astype(jnp.bfloat16)

def reference(fibre_records, station_records, band_mask, station_valid, segment_keep):
    dft_table = time_table()
    fibre_spec = matmul(fibre_records.reshape(-1, SAMPLES), dft_table).reshape(CHANNELS, SEG, 2 * NFREQ).astype(jnp.bfloat16)
    station_spec = matmul(station_records.reshape(-1, SAMPLES), dft_table).reshape(STA, SEG, 2 * NFREQ)
    totals = lax.optimization_barrier(jnp.sum(station_spec * station_spec, axis=(1, 2)))
    bands = scale_rows(station_spec, totals, station_valid)
    cosines, sines = wave_tables(KCH)
    weights = band_mask.T.astype(jnp.float32)
    grouped = fibre_spec.reshape(N_GRP, KCH, SEG, 2 * NFREQ)
    filtered = lax.map(lambda block: wavenumber_filter(block, cosines, sines, weights), grouped)
    filtered = filtered.reshape(CHANNELS, SEG, 2 * NFREQ)
    kept = filtered * segment_keep.astype(jnp.bfloat16)[None, :, None]
    fibre_four = kept.reshape(CHANNELS, SEG, 2, NFREQ).astype(jnp.float32)
    band_four = bands.reshape(STA, SEG, 2, NFREQ).astype(jnp.float32)
    rotated = jnp.concatenate([-band_four[:, :, 1:], band_four[:, :, :1]], axis=2)
    real_out = jnp.einsum('cgpb,sgpb->bcs', fibre_four, band_four)
    imag_out = jnp.einsum('cgpb,sgpb->bcs', fibre_four, rotated)
    return jnp.stack([real_out, imag_out]) * (1.0 / math.sqrt(SEG * SAMPLES))
```

```python
import math

import jax
import jax.numpy as jnp
from jax import lax
from jax.sharding import PartitionSpec as P

SEG = 256
SAMPLES = 1536
NFREQ = 8
FIRST_BIN = 24
NPART = 4


def time_table():
    sample_index = jnp.arange(SAMPLES, dtype=jnp.int32)
    bin_index = FIRST_BIN + jnp.arange(NFREQ, dtype=jnp.int32)
    phase = sample_index[:, None] * bin_index[None, :] % SAMPLES
    angle = phase.astype(jnp.float32) * (2.0 * math.pi / SAMPLES)
    return jnp.concatenate([jnp.cos(angle), -jnp.sin(angle)], axis=1).astype(jnp.bfloat16)


def wave_tables(width):
    index = jnp.arange(width, dtype=jnp.int32)
    phase = index[:, None] * index[None, :] % width
    angle = phase.astype(jnp.float32) * (2.0 * math.pi / width)
    return (jnp.cos(angle).astype(jnp.bfloat16), jnp.sin(angle).astype(jnp.bfloat16))


def matmul(left, right):
    return jnp.dot(left, right, preferred_element_type=jnp.float32)


def matmul_nt(left, right):
    return lax.dot_general(
        left, right, (((1,), (1,)), ((), ())), preferred_element_type=jnp.float32
    )


def transform(records, dft_table):
    rows = records.shape[0]
    spec = lax.dot_general(
        dft_table,
        records.reshape(rows * SEG, SAMPLES),
        (((0,), (1,)), ((), ())),
        preferred_element_type=jnp.float32,
    )
    return spec.reshape(2, NFREQ, rows, SEG)


def spread_table():
    source = jnp.arange(512, dtype=jnp.int32)
    target = (source // 8 % 16) * 32 + (source // 128) * 8 + source % 8
    return (target[:, None] == jnp.arange(512, dtype=jnp.int32)[None, :]).astype(jnp.bfloat16)


def shards(fibre_records, station_records, band_mask, station_valid, segment_keep):
    dft_table = time_table()
    here = fibre_records.shape[0]
    count = lax.axis_size("chan")
    width = here * count
    bin_here = lax.axis_index("chan") // NPART
    fibre_spec = transform(fibre_records, dft_table).astype(jnp.bfloat16)
    station_spec = transform(station_records, dft_table)
    totals = jnp.sum(station_spec * station_spec, axis=(0, 1, 3))
    factor = lax.rsqrt(totals / (2 * SEG * NFREQ) + 1e-06) * station_valid.astype(jnp.float32)
    bands = (station_spec * factor[None, None, :, None]).astype(jnp.bfloat16)
    near = station_records.shape[0] // NPART
    fibre_send = jnp.broadcast_to(
        fibre_spec.transpose(1, 2, 0, 3)[:, None], (NFREQ, NPART, here, 2, SEG)
    )
    band_send = bands.reshape(2, NFREQ, NPART, near, SEG).transpose(1, 2, 3, 0, 4)
    send = jnp.concatenate([fibre_send, band_send], axis=2).reshape(count, here + near, 2 * SEG)
    got = lax.all_to_all(send, "chan", split_axis=0, concat_axis=0, tiled=True)
    fibre_all = got[:, :here].reshape(width, 2 * SEG)
    keep = segment_keep.astype(jnp.bfloat16)
    band_all = got[:, here:].reshape(count * near, 2, SEG) * keep[None, None, :]
    band_re = band_all.reshape(count * near, 2 * SEG)
    band_im = jnp.concatenate([-band_all[:, 1], band_all[:, 0]], axis=1)
    cross_re = matmul_nt(fibre_all, band_re).astype(jnp.bfloat16)
    cross_im = matmul_nt(fibre_all, band_im).astype(jnp.bfloat16)
    cosines, sines = wave_tables(width)
    weights = lax.dynamic_index_in_dim(band_mask, bin_here, 0, keepdims=False)
    weights = weights.astype(jnp.float32)[:, None]
    wave_re = ((matmul(cosines, cross_re) + matmul(sines, cross_im)) * weights).astype(jnp.bfloat16)
    wave_im = ((matmul(cosines, cross_im) - matmul(sines, cross_re)) * weights).astype(jnp.bfloat16)
    scale = 1.0 / (width * math.sqrt(SEG * SAMPLES))
    out_re = ((matmul(cosines, wave_re) - matmul(sines, wave_im)) * scale).astype(jnp.bfloat16)
    out_im = ((matmul(sines, wave_re) + matmul(cosines, wave_im)) * scale).astype(jnp.bfloat16)
    lanes = out_re.shape[1]
    back = jnp.concatenate(
        [out_re.reshape(count, here, lanes), out_im.reshape(count, here, lanes)], axis=1
    )
    back = lax.all_to_all(back, "chan", split_axis=0, concat_axis=0, tiled=True)
    spread = spread_table()
    pieces = back.reshape(NFREQ, NPART, 2 * here, lanes)
    halves = []
    for h in range(2):
        joined = jnp.concatenate([pieces[:, q, :, 128 * h : 128 * h + 128] for q in range(NPART)], axis=2)
        halves.append(matmul(joined.reshape(NFREQ * 2 * here, 512), spread))
    final = jnp.concatenate(halves, axis=1).reshape(NFREQ, 2, here, NPART * lanes)
    return final.transpose(1, 0, 2, 3)


def solution(mesh):
    placed = (P(("grp", "chan"), None, None), P("chan", None, None), P(), P("chan"), P())
    return jax.shard_map(
        shards,
        mesh=mesh,
        in_specs=placed,
        out_specs=P(None, None, ("grp", "chan"), None),
        check_vma=False,
    )
```

```python
import functools
import math

import jax
import jax.numpy as jnp
import numpy as np
from jax import lax
from jax.experimental import pallas as pl
from jax.experimental.pallas import tpu as pltpu
from jax.sharding import PartitionSpec as P

SEG = 256
SAMPLES = 1536
NFREQ = 8
FIRST_BIN = 24
NPART = 4
PER_STEP = 2


def time_table():
    phase = (np.arange(SAMPLES)[None, :] * (FIRST_BIN + np.arange(NFREQ))[:, None]) % SAMPLES
    angle = phase.astype(np.float32) * np.float32(2.0 * math.pi / SAMPLES)
    return jnp.asarray(np.concatenate([np.cos(angle), -np.sin(angle)], axis=0), jnp.bfloat16)


def wave_tables(width):
    phase = (np.arange(width)[:, None] * np.arange(width)[None, :]) % width
    angle = phase.astype(np.float32) * np.float32(2.0 * math.pi / width)
    return (jnp.asarray(np.cos(angle), jnp.bfloat16), jnp.asarray(np.sin(angle), jnp.bfloat16))


def spread_table():
    source = np.arange(512)
    target = (source // 8 % 16) * 32 + (source // 128) * 8 + source % 8
    return jnp.asarray((target[:, None] == np.arange(512)[None, :]), jnp.bfloat16)


def matmul(left, right):
    return jnp.dot(left, right, preferred_element_type=jnp.float32)


def matmul_nt(left, right):
    return lax.dot_general(
        left, right, (((1,), (1,)), ((), ())), preferred_element_type=jnp.float32
    )


def spectra_kernel(fibre_steps, valid_ref, table_ref, fibre_ref, station_ref, out_ref, fibre_spec, station_spec):
    step = pl.program_id(0)
    table = table_ref[...]

    @pl.when(step < fibre_steps)
    def _():
        spec = matmul_nt(table, fibre_ref[...].reshape(PER_STEP * SEG, SAMPLES))
        for i in range(PER_STEP):
            fibre_spec[:, step * PER_STEP + i, :] = spec[:, i * SEG : (i + 1) * SEG]

    @pl.when(step >= fibre_steps)
    def _():
        spec = matmul_nt(table, station_ref[...].reshape(PER_STEP * SEG, SAMPLES))
        for i in range(PER_STEP):
            row = (step - fibre_steps) * PER_STEP + i
            part = spec[:, i * SEG : (i + 1) * SEG]
            total = jnp.sum(part * part, axis=(0, 1), keepdims=True)
            factor = lax.rsqrt(total / (2 * SEG * NFREQ) + 1e-06) * valid_ref[row].astype(jnp.float32)
            station_spec[:, row, :] = part * factor

    @pl.when(step == pl.num_programs(0) - 1)
    def _():
        near = station_spec.shape[1] // NPART
        for q in range(NPART):
            for b in range(0, NFREQ, 2):
                rows = pl.ds((q * NFREQ + b) * near, 2 * near)
                for p in range(2):
                    for source, first, base in (
                        (fibre_spec, 0, 0),
                        (station_spec, q * near, 2 * SEG),
                    ):
                        k = p * NFREQ + b
                        pair = jnp.concatenate(
                            [source[k, first : first + near, :], source[k + 1, first : first + near, :]],
                            axis=0,
                        )
                        out_ref[rows, base + p * SEG : base + (p + 1) * SEG] = pair.astype(jnp.bfloat16)


def band_spectra(fibre_records, station_records, station_valid):
    fibres, stations = fibre_records.shape[0], station_records.shape[0]
    fibre_steps, station_steps = fibres // PER_STEP, stations // PER_STEP
    rows = NPART * NFREQ * fibres
    return pl.pallas_call(
        functools.partial(spectra_kernel, fibre_steps),
        grid=(fibre_steps + station_steps,),
        in_specs=[
            pl.BlockSpec(memory_space=pltpu.SMEM),
            pl.BlockSpec((2 * NFREQ, SAMPLES), lambda i: (0, 0)),
            pl.BlockSpec((PER_STEP, SEG, SAMPLES), lambda i: (jnp.minimum(i, fibre_steps - 1), 0, 0)),
            pl.BlockSpec((PER_STEP, SEG, SAMPLES), lambda i: (jnp.maximum(i - fibre_steps, 0), 0, 0)),
        ],
        out_specs=pl.BlockSpec((rows, 4 * SEG), lambda i: (0, 0)),
        out_shape=jax.ShapeDtypeStruct((rows, 4 * SEG), jnp.bfloat16),
        scratch_shapes=[
            pltpu.VMEM((2 * NFREQ, fibres, SEG), jnp.float32),
            pltpu.VMEM((2 * NFREQ, stations, SEG), jnp.float32),
        ],
        name="band_spectra",
    )(station_valid, time_table(), fibre_records, station_records)


def cross_kernel(got_ref, keep_ref, mask_ref, cos_ref, sin_ref, out_ref):
    width = got_ref.shape[0]
    bin_here = lax.rem(lax.axis_index("chan"), NFREQ)
    fibre = got_ref[:, : 2 * SEG]
    keep = keep_ref[...].astype(jnp.bfloat16)
    band_re = got_ref[:, 2 * SEG : 3 * SEG] * keep
    band_im = got_ref[:, 3 * SEG :] * keep
    cross_re = matmul_nt(fibre, jnp.concatenate([band_re, band_im], axis=1)).astype(jnp.bfloat16)
    cross_im = matmul_nt(fibre, jnp.concatenate([-band_im, band_re], axis=1)).astype(jnp.bfloat16)
    cosines, sines = cos_ref[...], sin_ref[...]
    wave_re = (matmul(cosines, cross_re) + matmul(sines, cross_im)).astype(jnp.bfloat16)
    wave_im = (matmul(cosines, cross_im) - matmul(sines, cross_re)).astype(jnp.bfloat16)
    weights = mask_ref[pl.ds(bin_here, 1), :].astype(jnp.bfloat16)
    cosines, sines = cosines * weights, sines * weights
    scale = 1.0 / (width * math.sqrt(SEG * SAMPLES))
    out_re = (matmul(cosines, wave_re) - matmul(sines, wave_im)) * scale
    out_im = (matmul(sines, wave_re) + matmul(cosines, wave_im)) * scale
    lanes = out_re.shape[1]
    out_ref[:, :lanes] = out_re.astype(jnp.bfloat16)
    out_ref[:, lanes:] = out_im.astype(jnp.bfloat16)


def filtered_cross(got, segment_keep, band_mask):
    width = got.shape[0]
    cosines, sines = wave_tables(width)
    return pl.pallas_call(
        cross_kernel,
        out_shape=jax.ShapeDtypeStruct((width, 2 * SEG), jnp.bfloat16),
        name="filtered_cross",
    )(got, segment_keep.reshape(1, SEG), band_mask, cosines, sines)


def spread_kernel(got_ref, spread_ref, out_ref):
    rows = got_ref.shape[0] // NPART
    here = rows // NFREQ
    spread = spread_ref[...]
    for p in range(2):
        for h in range(2):
            lane = p * SEG + h * 128
            joined = jnp.concatenate(
                [got_ref[q * rows : (q + 1) * rows, lane : lane + 128] for q in range(NPART)], axis=1
            )
            part = matmul(joined, spread)
            out_ref[p, :, :, h * 512 : (h + 1) * 512] = part.reshape(NFREQ, here, 512)


def spread_out(got, here):
    return pl.pallas_call(
        spread_kernel,
        out_shape=jax.ShapeDtypeStruct((2, NFREQ, here, NPART * SEG), jnp.float32),
        name="spread_out",
    )(got, spread_table())


def exchange(rows, count):
    lanes = rows.shape[1]
    blocks = rows.reshape(count, rows.shape[0] // count, lanes)
    return lax.all_to_all(blocks, "chan", split_axis=0, concat_axis=0, tiled=True).reshape(rows.shape)


def shards(fibre_records, station_records, band_mask, station_valid, segment_keep):
    count = lax.axis_size("chan")
    here = fibre_records.shape[0]
    send = band_spectra(fibre_records, station_records, station_valid)
    got = exchange(send, count)
    back = filtered_cross(got, segment_keep, band_mask)
    return spread_out(exchange(back, count), here)


def solution(mesh):
    placed = (P(("grp", "chan"), None, None), P("chan", None, None), P(), P("chan"), P())
    return jax.shard_map(
        shards,
        mesh=mesh,
        in_specs=placed,
        out_specs=P(None, None, ("grp", "chan"), None),
        check_vma=False,
    )
```

```python
import functools
import math

import jax
import jax.numpy as jnp
import numpy as np
from jax import lax
from jax.experimental import pallas as pl
from jax.experimental.pallas import tpu as pltpu
from jax.sharding import PartitionSpec as P

SEG = 256
SAMPLES = 1536
NFREQ = 8
FIRST_BIN = 24
NPART = 4
PER_STEP = 4
AHEAD = 20


def time_table():
    phase = (np.arange(SAMPLES)[None, :] * (FIRST_BIN + np.arange(NFREQ))[:, None]) % SAMPLES
    angle = phase.astype(np.float32) * np.float32(2.0 * math.pi / SAMPLES)
    return jnp.asarray(np.concatenate([np.cos(angle), -np.sin(angle)], axis=0), jnp.bfloat16)


def wave_tables(width):
    phase = (np.arange(width)[:, None] * np.arange(width)[None, :]) % width
    angle = phase.astype(np.float32) * np.float32(2.0 * math.pi / width)
    return (jnp.asarray(np.cos(angle), jnp.bfloat16), jnp.asarray(np.sin(angle), jnp.bfloat16))


def spread_table():
    source = np.arange(512)
    target = (source // 8 % 16) * 32 + (source // 128) * 8 + source % 8
    return jnp.asarray((target[:, None] == np.arange(512)[None, :]), jnp.bfloat16)


def matmul(left, right):
    return jnp.dot(left, right, preferred_element_type=jnp.float32)


def matmul_nt(left, right):
    return lax.dot_general(
        left, right, (((1,), (1,)), ((), ())), preferred_element_type=jnp.float32
    )


def spectra_kernel(valid_ref, table_ref, fibre_ref, station_ref, out_ref, slab, held, arrived):
    items = slab.shape[0]

    def copy(records_ref, row, item):
        return pltpu.make_async_copy(records_ref.at[row], slab.at[item], arrived.at[item])

    def start(item):
        if item < 8:
            copy(fibre_ref, item, item).start()
        elif item < items:
            copy(station_ref, item - 8, item).start()

    def gather(records_ref, first, ahead):
        for j in range(0, 8, PER_STEP):
            for i in range(j, j + PER_STEP):
                copy(records_ref, first - (0 if records_ref is fibre_ref else 8) + i, first + i).wait()
                ahead(i)
            records = slab[pl.ds(first + j, PER_STEP)].reshape(PER_STEP * SEG, SAMPLES)
            spec = matmul_nt(table_ref[...], records)
            for i in range(PER_STEP):
                held[:, j + i, :] = spec[:, i * SEG : (i + 1) * SEG]
        return [held[k] for k in range(2 * NFREQ)]

    def store(quarter, base, spectra):
        for b in range(0, NFREQ, 2):
            for p in range(2):
                k = p * NFREQ + b
                pair = jnp.concatenate([spectra[k], spectra[k + 1]], axis=0).astype(jnp.bfloat16)
                first = pl.multiple_of((quarter * NFREQ + b) * 8, 16)
                out_ref[pl.ds(first, 16), base + p * SEG : base + (p + 1) * SEG] = pair

    for item in range(AHEAD):
        start(item)
    spectra = gather(fibre_ref, 0, lambda i: start(i + AHEAD))
    for q in range(NPART):
        store(q, 0, spectra)

    def stations(q, carry):
        first = 8 + q * 8

        def ahead(i):
            @pl.when(first + i + AHEAD < items)
            def _():
                copy(station_ref, first + i + AHEAD - 8, first + i + AHEAD).start()

        spectra = gather(station_ref, first, ahead)
        totals = jnp.sum(sum(tile * tile for tile in spectra), axis=1, keepdims=True)
        place = lax.broadcasted_iota(jnp.int32, (8, 1), 0)
        valid = jnp.zeros((8, 1), jnp.float32)
        for i in range(8):
            valid = jnp.where(place == i, valid_ref[q * 8 + i].astype(jnp.float32), valid)
        factor = lax.rsqrt(totals / (2 * SEG * NFREQ) + 1e-06) * valid
        store(q, 2 * SEG, [tile * factor for tile in spectra])
        return carry

    lax.fori_loop(0, NPART, stations, 0)


def band_spectra(fibre_records, station_records, station_valid):
    items = fibre_records.shape[0] + station_records.shape[0]
    rows = NPART * NFREQ * 8
    return pl.pallas_call(
        spectra_kernel,
        in_specs=[
            pl.BlockSpec(memory_space=pltpu.SMEM),
            pl.BlockSpec(memory_space=pltpu.VMEM),
            pl.BlockSpec(memory_space=pl.ANY),
            pl.BlockSpec(memory_space=pl.ANY),
        ],
        out_specs=pl.BlockSpec(memory_space=pltpu.VMEM),
        out_shape=jax.ShapeDtypeStruct((rows, 4 * SEG), jnp.bfloat16),
        scratch_shapes=[
            pltpu.VMEM((items, SEG, SAMPLES), jnp.bfloat16),
            pltpu.VMEM((2 * NFREQ, 8, SEG), jnp.float32),
            pltpu.SemaphoreType.DMA((items,)),
        ],
        compiler_params=pltpu.CompilerParams(vmem_limit_bytes=52 << 20),
        name="band_spectra",
    )(station_valid, time_table(), fibre_records, station_records)


def cross_kernel(got_ref, keep_ref, mask_ref, cos_ref, sin_ref, out_ref):
    width = got_ref.shape[0]
    bin_here = lax.rem(lax.axis_index("chan"), NFREQ)
    fibre = got_ref[:, : 2 * SEG]
    keep = keep_ref[...].astype(jnp.bfloat16)
    band_re = got_ref[:, 2 * SEG : 3 * SEG] * keep
    band_im = got_ref[:, 3 * SEG :] * keep
    cross_re = matmul_nt(fibre, jnp.concatenate([band_re, band_im], axis=1)).astype(jnp.bfloat16)
    cross_im = matmul_nt(fibre, jnp.concatenate([-band_im, band_re], axis=1)).astype(jnp.bfloat16)
    cosines, sines = cos_ref[...], sin_ref[...]
    wave_re = (matmul(cosines, cross_re) + matmul(sines, cross_im)).astype(jnp.bfloat16)
    wave_im = (matmul(cosines, cross_im) - matmul(sines, cross_re)).astype(jnp.bfloat16)
    weights = mask_ref[pl.ds(bin_here, 1), :].astype(jnp.bfloat16)
    cosines, sines = cosines * weights, sines * weights
    scale = 1.0 / (width * math.sqrt(SEG * SAMPLES))
    out_re = (matmul(cosines, wave_re) - matmul(sines, wave_im)) * scale
    out_im = (matmul(sines, wave_re) + matmul(cosines, wave_im)) * scale
    lanes = out_re.shape[1]
    out_ref[:, :lanes] = out_re.astype(jnp.bfloat16)
    out_ref[:, lanes:] = out_im.astype(jnp.bfloat16)


def filtered_cross(got, segment_keep, band_mask):
    width = got.shape[0]
    cosines, sines = wave_tables(width)
    return pl.pallas_call(
        cross_kernel,
        out_shape=jax.ShapeDtypeStruct((width, 2 * SEG), jnp.bfloat16),
        compiler_params=pltpu.CompilerParams(vmem_limit_bytes=12 << 20),
        name="filtered_cross",
    )(got, segment_keep.reshape(1, SEG), band_mask, cosines, sines)


def spread_kernel(got_ref, spread_ref, out_ref):
    rows = got_ref.shape[0] // NPART
    here = rows // NFREQ
    spread = spread_ref[...]
    for p in range(2):
        for h in range(2):
            lane = p * SEG + h * 128
            joined = jnp.concatenate(
                [got_ref[q * rows : (q + 1) * rows, lane : lane + 128] for q in range(NPART)], axis=1
            )
            part = matmul(joined, spread)
            out_ref[p, :, :, h * 512 : (h + 1) * 512] = part.reshape(NFREQ, here, 512)


def spread_out(got, here):
    return pl.pallas_call(
        spread_kernel,
        out_shape=jax.ShapeDtypeStruct((2, NFREQ, here, NPART * SEG), jnp.float32),
        compiler_params=pltpu.CompilerParams(vmem_limit_bytes=12 << 20),
        name="spread_out",
    )(got, spread_table())


def exchange(rows, count):
    lanes = rows.shape[1]
    blocks = rows.reshape(count, rows.shape[0] // count, lanes)
    return lax.all_to_all(blocks, "chan", split_axis=0, concat_axis=0, tiled=True).reshape(rows.shape)


def shards(fibre_records, station_records, band_mask, station_valid, segment_keep):
    count = lax.axis_size("chan")
    here = fibre_records.shape[0]
    send = band_spectra(fibre_records, station_records, station_valid)
    got = exchange(send, count)
    back = filtered_cross(got, segment_keep, band_mask)
    return spread_out(exchange(back, count), here)


def solution(mesh):
    placed = (P(("grp", "chan"), None, None), P("chan", None, None), P(), P("chan"), P())
    return jax.shard_map(
        shards,
        mesh=mesh,
        in_specs=placed,
        out_specs=P(None, None, ("grp", "chan"), None),
        check_vma=False,
    )
```

```python
import math

import jax
import jax.numpy as jnp
import numpy as np
from jax import lax
from jax.experimental import pallas as pl
from jax.experimental.pallas import tpu as pltpu
from jax.sharding import PartitionSpec as P


SEG = 256
SAMPLES = 1536
NFREQ = 8
FIRST_BIN = 24
NPART = 4
PER_STEP = 4
AHEAD = 20


def time_table():
    phase = (np.arange(SAMPLES)[None, :] * (FIRST_BIN + np.arange(NFREQ))[:, None]) % SAMPLES
    angle = phase.astype(np.float32) * np.float32(2.0 * math.pi / SAMPLES)
    return jnp.asarray(np.concatenate([np.cos(angle), -np.sin(angle)], axis=0), jnp.bfloat16)


def wave_tables(width):
    phase = (np.arange(width)[:, None] * np.arange(width)[None, :]) % width
    angle = phase.astype(np.float32) * np.float32(2.0 * math.pi / width)
    return (jnp.asarray(np.cos(angle), jnp.bfloat16), jnp.asarray(np.sin(angle), jnp.bfloat16))


def matmul(left, right):
    return jnp.dot(left, right, preferred_element_type=jnp.float32)


def matmul_nt(left, right):
    return lax.dot_general(
        left, right, (((1,), (1,)), ((), ())), preferred_element_type=jnp.float32
    )


def gather(records_ref, table_ref, slab, held, arrived, first, count):
    items = slab.shape[0]
    for j in range(0, count, PER_STEP):
        for i in range(j, j + PER_STEP):
            record_copy(records_ref, slab, arrived, first + i).wait()

            if items > AHEAD:

                @pl.when(first + i + AHEAD < items)
                def _():
                    record_copy(records_ref, slab, arrived, first + i + AHEAD).start()

        records = slab[pl.ds(first + j, PER_STEP)].reshape(PER_STEP * SEG, SAMPLES)
        spec = matmul_nt(table_ref[...], records)
        for i in range(PER_STEP):
            held[:, j + i, :] = spec[:, i * SEG : (i + 1) * SEG]
    return [held[k] for k in range(2 * NFREQ)]


def record_copy(records_ref, slab, arrived, item):
    return pltpu.make_async_copy(records_ref.at[item], slab.at[item], arrived.at[item])


def fibre_kernel(table_in, records_ref, out_ref, slab, held, arrived, table_ref, small):
    here = slab.shape[0]
    table_copy = pltpu.make_async_copy(table_in, table_ref, small.at[0])
    table_copy.start()
    for item in range(min(AHEAD, here)):
        record_copy(records_ref, slab, arrived, item).start()
    table_copy.wait()
    spectra = gather(records_ref, table_ref, slab, held, arrived, 0, here)
    for b in range(0, NFREQ, 2):
        for p in range(2):
            k = p * NFREQ + b
            pair = jnp.concatenate([spectra[k], spectra[k + 1]], axis=0).astype(jnp.bfloat16)
            for q in range(NPART):
                first = (q * NFREQ + b) * here
                out_ref[first : first + 2 * here, p * SEG : (p + 1) * SEG] = pair


def station_kernel(valid_in, table_in, records_ref, out_ref, slab, held, arrived, table_ref, small, valid_ref):
    stations, batch = slab.shape[0], held.shape[1]
    table_copy = pltpu.make_async_copy(table_in, table_ref, small.at[0])
    valid_copy = pltpu.make_async_copy(valid_in, valid_ref, small.at[1])
    table_copy.start()
    valid_copy.start()
    for item in range(min(AHEAD, stations)):
        record_copy(records_ref, slab, arrived, item).start()
    table_copy.wait()
    valid_copy.wait()

    def step(turn, carry):
        first = pl.multiple_of(turn * batch, batch)
        spectra = gather(records_ref, table_ref, slab, held, arrived, first, batch)
        totals = jnp.sum(sum(tile * tile for tile in spectra), axis=1, keepdims=True)
        place = lax.broadcasted_iota(jnp.int32, (batch, 1), 0)
        valid = jnp.zeros((batch, 1), jnp.float32)
        for i in range(batch):
            valid = jnp.where(place == i, valid_ref[first + i].astype(jnp.float32), valid)
        factor = lax.rsqrt(totals / (2 * SEG * NFREQ) + 1e-06) * valid
        for p in range(2):
            for b in range(NFREQ):
                rows = pl.ds(pl.multiple_of(b * stations + first, batch), batch)
                band = (spectra[p * NFREQ + b] * factor).astype(jnp.bfloat16)
                out_ref[rows, p * SEG : (p + 1) * SEG] = band
        return carry

    lax.fori_loop(0, stations // batch, step, 0)


def spectra_call(kernel, records, flags, out_rows, batch, grant):
    rows = records.shape[0]
    return pl.pallas_call(
        kernel,
        in_specs=[pl.BlockSpec(memory_space=pl.ANY)] * (len(flags) + 2),
        out_specs=pl.BlockSpec(memory_space=pltpu.VMEM),
        out_shape=jax.ShapeDtypeStruct((out_rows, 2 * SEG), jnp.bfloat16),
        scratch_shapes=[
            pltpu.VMEM((rows, SEG, SAMPLES), jnp.bfloat16),
            pltpu.VMEM((2 * NFREQ, batch, SEG), jnp.float32),
            pltpu.SemaphoreType.DMA((rows,)),
            pltpu.VMEM((2 * NFREQ, SAMPLES), jnp.bfloat16),
            pltpu.SemaphoreType.DMA((2,)),
        ]
        + [pltpu.SMEM(flag.shape, flag.dtype) for flag in flags],
        cost_estimate=pl.CostEstimate(
            flops=rows * SEG * SAMPLES * 512, bytes_accessed=rows * SEG * SAMPLES * 2, transcendentals=0
        ),
        compiler_params=pltpu.CompilerParams(vmem_limit_bytes=grant << 20),
    )(*flags, time_table(), records)


def cross_kernel(fibre_ref, band_ref, keep_ref, mask_ref, cos_ref, sin_ref, out_ref):
    width = fibre_ref.shape[0]
    bin_here = lax.rem(lax.axis_index("chan"), NFREQ)
    fibre = fibre_ref[...]
    keep = keep_ref[...].astype(jnp.bfloat16)
    band_re = band_ref[:, :SEG] * keep
    band_im = band_ref[:, SEG:] * keep
    cross_re = matmul_nt(fibre, jnp.concatenate([band_re, band_im], axis=1)).astype(jnp.bfloat16)
    cross_im = matmul_nt(fibre, jnp.concatenate([-band_im, band_re], axis=1)).astype(jnp.bfloat16)
    cosines, sines = cos_ref[...], sin_ref[...]
    wave_re = (matmul(cosines, cross_re) + matmul(sines, cross_im)).astype(jnp.bfloat16)
    wave_im = (matmul(cosines, cross_im) - matmul(sines, cross_re)).astype(jnp.bfloat16)
    weights = mask_ref[pl.ds(bin_here, 1), :].astype(jnp.bfloat16)
    cosines, sines = cosines * weights, sines * weights
    scale = 1.0 / (width * math.sqrt(SEG * SAMPLES))
    out_re = (matmul(cosines, wave_re) - matmul(sines, wave_im)) * scale
    out_im = (matmul(sines, wave_re) + matmul(cosines, wave_im)) * scale
    lanes = out_re.shape[1]
    out_ref[:, :lanes] = out_re.astype(jnp.bfloat16)
    out_ref[:, lanes:] = out_im.astype(jnp.bfloat16)


def filtered_cross(fibre_got, band_got, segment_keep, band_mask):
    width = fibre_got.shape[0]
    cosines, sines = wave_tables(width)
    return pl.pallas_call(
        cross_kernel,
        out_shape=jax.ShapeDtypeStruct((width, 2 * SEG), jnp.bfloat16),
        compiler_params=pltpu.CompilerParams(vmem_limit_bytes=12 << 20),
        name="filtered_cross",
    )(fibre_got, band_got, segment_keep.reshape(1, SEG), band_mask, cosines, sines)


def place_kernel(got_ref, out_ref):
    rows = got_ref.shape[0] // NPART
    for q in range(NPART):
        for p in range(2):
            part = got_ref[q * rows : (q + 1) * rows, p * SEG : (p + 1) * SEG].astype(jnp.float32)
            out_ref[p, :, :, q * SEG : (q + 1) * SEG] = part.reshape(NFREQ, rows // NFREQ, SEG)


def place_out(got, here):
    return pl.pallas_call(
        place_kernel,
        out_shape=jax.ShapeDtypeStruct((2, NFREQ, here, NPART * SEG), jnp.float32),
        compiler_params=pltpu.CompilerParams(vmem_limit_bytes=12 << 20),
        name="place_out",
    )(got)


def exchange(rows, count, groups=None):
    lanes = rows.shape[1]
    blocks = rows.reshape(count, rows.shape[0] // count, lanes)
    blocks = lax.all_to_all(
        blocks, "chan", split_axis=0, concat_axis=0, tiled=True, axis_index_groups=groups
    )
    return blocks.reshape(rows.shape)


def shards(fibre_records, station_records, band_mask, station_valid, segment_keep):
    count = lax.axis_size("chan")
    here, stations = fibre_records.shape[0], station_records.shape[0]
    quarters = [[q * NFREQ + b for b in range(NFREQ)] for q in range(NPART)]
    fibre_send = spectra_call(fibre_kernel, fibre_records, (), count * here, here, 58)
    fibre_got = exchange(fibre_send, count)
    band_send = spectra_call(station_kernel, station_records, (station_valid,), NFREQ * stations, 16, 58)
    band_got = exchange(band_send, NFREQ, quarters)
    back = filtered_cross(fibre_got, band_got, segment_keep, band_mask)
    return place_out(exchange(back, count), here)


def solution(mesh):
    placed = (P(("grp", "chan"), None, None), P("chan", None, None), P(), P("chan"), P())
    return jax.shard_map(
        shards,
        mesh=mesh,
        in_specs=placed,
        out_specs=P(None, None, ("grp", "chan"), None),
        check_vma=False,
    )
```

```python
import math

import jax
import jax.numpy as jnp
import numpy as np
from jax import lax
from jax.experimental import pallas as pl
from jax.experimental.pallas import tpu as pltpu
from jax.sharding import PartitionSpec as P


SEG = 256
SAMPLES = 1536
NFREQ = 8
FIRST_BIN = 24
NPART = 4
PER_STEP = 4
AHEAD = 10
INIT = 4


def time_table():
    phase = (np.arange(SAMPLES)[None, :] * (FIRST_BIN + np.arange(NFREQ))[:, None]) % SAMPLES
    angle = phase.astype(np.float32) * np.float32(2.0 * math.pi / SAMPLES)
    return jnp.asarray(np.concatenate([np.cos(angle), -np.sin(angle)], axis=0), jnp.bfloat16)


def wave_tables(width):
    phase = (np.arange(width)[:, None] * np.arange(width)[None, :]) % width
    angle = phase.astype(np.float32) * np.float32(2.0 * math.pi / width)
    return (jnp.asarray(np.cos(angle), jnp.bfloat16), jnp.asarray(np.sin(angle), jnp.bfloat16))


def matmul(left, right):
    return jnp.dot(left, right, preferred_element_type=jnp.float32)


def matmul_nt(left, right):
    return lax.dot_general(
        left, right, (((1,), (1,)), ((), ())), preferred_element_type=jnp.float32
    )


def gather(records_ref, table_ref, slab, held, arrived, first, count):
    items = slab.shape[0]
    for j in range(0, count, PER_STEP):
        for i in range(j, j + PER_STEP):
            record_copy(records_ref, slab, arrived, first + i).wait()

            if items > AHEAD:

                @pl.when(first + i + AHEAD < items)
                def _():
                    record_copy(records_ref, slab, arrived, first + i + AHEAD).start()

        records = slab[pl.ds(first + j, PER_STEP)].reshape(PER_STEP * SEG, SAMPLES)
        spec = matmul_nt(table_ref[...], records)
        for i in range(PER_STEP):
            held[:, j + i, :] = spec[:, i * SEG : (i + 1) * SEG]
    return [held[k] for k in range(2 * NFREQ)]


def record_copy(records_ref, slab, arrived, item):
    return pltpu.make_async_copy(records_ref.at[item], slab.at[item], arrived.at[item])


def fibre_kernel(table_in, records_ref, out_ref, slab, held, arrived, table_ref, small):
    here = slab.shape[0]
    table_copy = pltpu.make_async_copy(table_in, table_ref, small.at[0])
    table_copy.start()
    for item in range(min(INIT, here)):
        record_copy(records_ref, slab, arrived, item).start()
    table_copy.wait()
    for item in range(INIT, min(AHEAD, here)):
        record_copy(records_ref, slab, arrived, item).start()
    spectra = gather(records_ref, table_ref, slab, held, arrived, 0, here)
    for b in range(0, NFREQ, 2):
        for p in range(2):
            k = p * NFREQ + b
            pair = jnp.concatenate([spectra[k], spectra[k + 1]], axis=0).astype(jnp.bfloat16)
            for q in range(NPART):
                first = (q * NFREQ + b) * here
                out_ref[first : first + 2 * here, p * SEG : (p + 1) * SEG] = pair


def station_kernel(valid_in, table_in, records_ref, out_ref, slab, held, arrived, table_ref, small, valid_ref):
    stations, batch = slab.shape[0], held.shape[1]
    table_copy = pltpu.make_async_copy(table_in, table_ref, small.at[0])
    valid_copy = pltpu.make_async_copy(valid_in, valid_ref, small.at[1])
    table_copy.start()
    valid_copy.start()
    for item in range(min(INIT, stations)):
        record_copy(records_ref, slab, arrived, item).start()
    table_copy.wait()
    for item in range(INIT, min(AHEAD, stations)):
        record_copy(records_ref, slab, arrived, item).start()

    def step(turn, carry):
        first = pl.multiple_of(turn * batch, batch)
        spectra = gather(records_ref, table_ref, slab, held, arrived, first, batch)

        @pl.when(turn == 0)
        def _():
            valid_copy.wait()

        totals = jnp.sum(sum(tile * tile for tile in spectra), axis=1, keepdims=True)
        place = lax.broadcasted_iota(jnp.int32, (batch, 1), 0)
        valid = jnp.zeros((batch, 1), jnp.float32)
        for i in range(batch):
            valid = jnp.where(place == i, valid_ref[first + i].astype(jnp.float32), valid)
        factor = lax.rsqrt(totals / (2 * SEG * NFREQ) + 1e-06) * valid
        for p in range(2):
            for b in range(NFREQ):
                rows = pl.ds(pl.multiple_of(b * stations + first, batch), batch)
                band = (spectra[p * NFREQ + b] * factor).astype(jnp.bfloat16)
                out_ref[rows, p * SEG : (p + 1) * SEG] = band
        return carry

    lax.fori_loop(0, stations // batch, step, 0)


def spectra_call(kernel, records, flags, out_rows, batch, grant):
    rows = records.shape[0]
    return pl.pallas_call(
        kernel,
        in_specs=[pl.BlockSpec(memory_space=pl.ANY)] * (len(flags) + 2),
        out_specs=pl.BlockSpec(memory_space=pltpu.VMEM),
        out_shape=jax.ShapeDtypeStruct((out_rows, 2 * SEG), jnp.bfloat16),
        scratch_shapes=[
            pltpu.VMEM((rows, SEG, SAMPLES), jnp.bfloat16),
            pltpu.VMEM((2 * NFREQ, batch, SEG), jnp.float32),
            pltpu.SemaphoreType.DMA((rows,)),
            pltpu.VMEM((2 * NFREQ, SAMPLES), jnp.bfloat16),
            pltpu.SemaphoreType.DMA((2,)),
        ]
        + [pltpu.SMEM(flag.shape, flag.dtype) for flag in flags],
        cost_estimate=pl.CostEstimate(
            flops=rows * SEG * SAMPLES * 512, bytes_accessed=rows * SEG * SAMPLES * 2, transcendentals=0
        ),
        compiler_params=pltpu.CompilerParams(vmem_limit_bytes=grant << 20),
    )(*flags, time_table(), records)


def cross_kernel(fibre_ref, band_ref, keep_ref, mask_ref, cos_ref, sin_ref, out_ref):
    width = fibre_ref.shape[0]
    bin_here = lax.rem(lax.axis_index("chan"), NFREQ)
    fibre = fibre_ref[...]
    keep = keep_ref[...].astype(jnp.bfloat16)
    band_re = band_ref[:, :SEG] * keep
    band_im = band_ref[:, SEG:] * keep
    cross_re = matmul_nt(fibre, jnp.concatenate([band_re, band_im], axis=1)).astype(jnp.bfloat16)
    cross_im = matmul_nt(fibre, jnp.concatenate([-band_im, band_re], axis=1)).astype(jnp.bfloat16)
    cosines, sines = cos_ref[...], sin_ref[...]
    wave_re = (matmul(cosines, cross_re) + matmul(sines, cross_im)).astype(jnp.bfloat16)
    wave_im = (matmul(cosines, cross_im) - matmul(sines, cross_re)).astype(jnp.bfloat16)
    weights = mask_ref[pl.ds(bin_here, 1), :].astype(jnp.bfloat16)
    cosines, sines = cosines * weights, sines * weights
    scale = 1.0 / (width * math.sqrt(SEG * SAMPLES))
    out_re = (matmul(cosines, wave_re) - matmul(sines, wave_im)) * scale
    out_im = (matmul(sines, wave_re) + matmul(cosines, wave_im)) * scale
    lanes = out_re.shape[1]
    out_ref[:, :lanes] = out_re.astype(jnp.bfloat16)
    out_ref[:, lanes:] = out_im.astype(jnp.bfloat16)


def filtered_cross(fibre_got, band_got, segment_keep, band_mask):
    width = fibre_got.shape[0]
    cosines, sines = wave_tables(width)
    return pl.pallas_call(
        cross_kernel,
        out_shape=jax.ShapeDtypeStruct((width, 2 * SEG), jnp.bfloat16),
        compiler_params=pltpu.CompilerParams(vmem_limit_bytes=12 << 20),
        name="filtered_cross",
    )(fibre_got, band_got, segment_keep.reshape(1, SEG), band_mask, cosines, sines)


def place_kernel(got_ref, out_ref):
    rows = got_ref.shape[0] // NPART
    for q in range(NPART):
        for p in range(2):
            part = got_ref[q * rows : (q + 1) * rows, p * SEG : (p + 1) * SEG].astype(jnp.float32)
            out_ref[p, :, :, q * SEG : (q + 1) * SEG] = part.reshape(NFREQ, rows // NFREQ, SEG)


def place_out(got, here):
    return pl.pallas_call(
        place_kernel,
        out_shape=jax.ShapeDtypeStruct((2, NFREQ, here, NPART * SEG), jnp.float32),
        compiler_params=pltpu.CompilerParams(vmem_limit_bytes=12 << 20),
        name="place_out",
    )(got)


def exchange(rows, count, groups=None):
    lanes = rows.shape[1]
    blocks = rows.reshape(count, rows.shape[0] // count, lanes)
    blocks = lax.all_to_all(
        blocks, "chan", split_axis=0, concat_axis=0, tiled=True, axis_index_groups=groups
    )
    return blocks.reshape(rows.shape)


def shards(fibre_records, station_records, band_mask, station_valid, segment_keep):
    count = lax.axis_size("chan")
    here, stations = fibre_records.shape[0], station_records.shape[0]
    quarters = [[q * NFREQ + b for b in range(NFREQ)] for q in range(NPART)]
    fibre_send = spectra_call(fibre_kernel, fibre_records, (), count * here, here, 58)
    fibre_got = exchange(fibre_send, count)
    band_send = spectra_call(station_kernel, station_records, (station_valid,), NFREQ * stations, 16, 58)
    band_got = exchange(band_send, NFREQ, quarters)
    back = filtered_cross(fibre_got, band_got, segment_keep, band_mask)
    return place_out(exchange(back, count), here)


def solution(mesh):
    placed = (P(("grp", "chan"), None, None), P("chan", None, None), P(), P("chan"), P())
    return jax.shard_map(
        shards,
        mesh=mesh,
        in_specs=placed,
        out_specs=P(None, None, ("grp", "chan"), None),
        check_vma=False,
    )
```

```python
import math

import jax
import jax.numpy as jnp
import numpy as np
from jax import lax
from jax.experimental import pallas as pl
from jax.experimental.pallas import tpu as pltpu
from jax.sharding import PartitionSpec as P


SEG = 256
SAMPLES = 1536
NFREQ = 8
FIRST_BIN = 24
NPART = 4
FIBRE_CHUNKS = (4, 2, 2)
STATION_CHUNKS = (4, 4, 4, 4)
AHEAD = 8
INIT = 4


def time_table():
    phase = (np.arange(SAMPLES)[None, :] * (FIRST_BIN + np.arange(NFREQ))[:, None]) % SAMPLES
    angle = phase.astype(np.float32) * np.float32(2.0 * math.pi / SAMPLES)
    return jnp.asarray(np.concatenate([np.cos(angle), -np.sin(angle)], axis=0), jnp.bfloat16)


def wave_tables(width):
    phase = (np.arange(width)[:, None] * np.arange(width)[None, :]) % width
    angle = phase.astype(np.float32) * np.float32(2.0 * math.pi / width)
    return (jnp.asarray(np.cos(angle), jnp.bfloat16), jnp.asarray(np.sin(angle), jnp.bfloat16))


def matmul(left, right):
    return jnp.dot(left, right, preferred_element_type=jnp.float32)


def matmul_nt(left, right):
    return lax.dot_general(
        left, right, (((1,), (1,)), ((), ())), preferred_element_type=jnp.float32
    )


def gather(records_ref, table_ref, slab, held, arrived, first, chunks):
    items = slab.shape[0]
    j = 0
    for size in chunks:
        for i in range(j, j + size):
            record_copy(records_ref, slab, arrived, first + i).wait()
            if items > AHEAD:

                @pl.when(first + i + AHEAD < items)
                def _():
                    record_copy(records_ref, slab, arrived, first + i + AHEAD).start()

        records = slab[pl.ds(first + j, size)].reshape(size * SEG, SAMPLES)
        spec = matmul_nt(table_ref[...], records)
        for i in range(size):
            held[:, j + i, :] = spec[:, i * SEG : (i + 1) * SEG]
        j += size
    return [held[k] for k in range(2 * NFREQ)]


def record_copy(records_ref, slab, arrived, item):
    return pltpu.make_async_copy(records_ref.at[item], slab.at[item], arrived.at[item])


def fibre_kernel(table_in, records_ref, out_ref, slab, held, arrived, table_ref, small):
    here = slab.shape[0]
    table_copy = pltpu.make_async_copy(table_in, table_ref, small.at[0])
    table_copy.start()
    for item in range(min(INIT, here)):
        record_copy(records_ref, slab, arrived, item).start()
    table_copy.wait()
    for item in range(INIT, min(AHEAD, here)):
        record_copy(records_ref, slab, arrived, item).start()
    spectra = gather(records_ref, table_ref, slab, held, arrived, 0, FIBRE_CHUNKS)
    for b in range(0, NFREQ, 2):
        for p in range(2):
            k = p * NFREQ + b
            pair = jnp.concatenate([spectra[k], spectra[k + 1]], axis=0).astype(jnp.bfloat16)
            for q in range(NPART):
                first = (q * NFREQ + b) * here
                out_ref[first : first + 2 * here, p * SEG : (p + 1) * SEG] = pair


def station_kernel(valid_in, table_in, records_ref, out_ref, slab, held, arrived, table_ref, small, valid_ref):
    stations, batch = slab.shape[0], held.shape[1]
    table_copy = pltpu.make_async_copy(table_in, table_ref, small.at[0])
    valid_copy = pltpu.make_async_copy(valid_in, valid_ref, small.at[1])
    table_copy.start()
    valid_copy.start()
    for item in range(min(INIT, stations)):
        record_copy(records_ref, slab, arrived, item).start()
    table_copy.wait()
    for item in range(INIT, min(AHEAD, stations)):
        record_copy(records_ref, slab, arrived, item).start()

    def step(turn, carry):
        first = pl.multiple_of(turn * batch, batch)
        spectra = gather(records_ref, table_ref, slab, held, arrived, first, STATION_CHUNKS)

        @pl.when(turn == 0)
        def _():
            valid_copy.wait()

        totals = jnp.sum(sum(tile * tile for tile in spectra), axis=1, keepdims=True)
        place = lax.broadcasted_iota(jnp.int32, (batch, 1), 0)
        valid = jnp.zeros((batch, 1), jnp.float32)
        for i in range(batch):
            valid = jnp.where(place == i, valid_ref[first + i].astype(jnp.float32), valid)
        factor = lax.rsqrt(totals / (2 * SEG * NFREQ) + 1e-06) * valid
        for p in range(2):
            for b in range(NFREQ):
                rows = pl.ds(pl.multiple_of(b * stations + first, batch), batch)
                band = (spectra[p * NFREQ + b] * factor).astype(jnp.bfloat16)
                out_ref[rows, p * SEG : (p + 1) * SEG] = band
        return carry

    lax.fori_loop(0, stations // batch, step, 0)


def spectra_call(kernel, records, flags, out_rows, batch, grant):
    rows = records.shape[0]
    return pl.pallas_call(
        kernel,
        in_specs=[pl.BlockSpec(memory_space=pl.ANY)] * (len(flags) + 2),
        out_specs=pl.BlockSpec(memory_space=pltpu.VMEM),
        out_shape=jax.ShapeDtypeStruct((out_rows, 2 * SEG), jnp.bfloat16),
        scratch_shapes=[
            pltpu.VMEM((rows, SEG, SAMPLES), jnp.bfloat16),
            pltpu.VMEM((2 * NFREQ, batch, SEG), jnp.float32),
            pltpu.SemaphoreType.DMA((rows,)),
            pltpu.VMEM((2 * NFREQ, SAMPLES), jnp.bfloat16),
            pltpu.SemaphoreType.DMA((2,)),
        ]
        + [pltpu.SMEM(flag.shape, flag.dtype) for flag in flags],
        cost_estimate=pl.CostEstimate(
            flops=rows * SEG * SAMPLES * 512, bytes_accessed=rows * SEG * SAMPLES * 2, transcendentals=0
        ),
        compiler_params=pltpu.CompilerParams(vmem_limit_bytes=grant << 20),
    )(*flags, time_table(), records)


def cross_kernel(fibre_ref, band_ref, keep_ref, mask_ref, cos_ref, sin_ref, out_ref):
    width = fibre_ref.shape[0]
    bin_here = lax.rem(lax.axis_index("chan"), NFREQ)
    fibre = fibre_ref[...]
    keep = keep_ref[...].astype(jnp.bfloat16)
    band_re = band_ref[:, :SEG] * keep
    band_im = band_ref[:, SEG:] * keep
    cross_re = matmul_nt(fibre, jnp.concatenate([band_re, band_im], axis=1)).astype(jnp.bfloat16)
    cross_im = matmul_nt(fibre, jnp.concatenate([-band_im, band_re], axis=1)).astype(jnp.bfloat16)
    cosines, sines = cos_ref[...], sin_ref[...]
    wave_re = (matmul(cosines, cross_re) + matmul(sines, cross_im)).astype(jnp.bfloat16)
    wave_im = (matmul(cosines, cross_im) - matmul(sines, cross_re)).astype(jnp.bfloat16)
    weights = mask_ref[pl.ds(bin_here, 1), :].astype(jnp.bfloat16)
    cosines, sines = cosines * weights, sines * weights
    scale = 1.0 / (width * math.sqrt(SEG * SAMPLES))
    out_re = (matmul(cosines, wave_re) - matmul(sines, wave_im)) * scale
    out_im = (matmul(sines, wave_re) + matmul(cosines, wave_im)) * scale
    lanes = out_re.shape[1]
    out_ref[:, :lanes] = out_re.astype(jnp.bfloat16)
    out_ref[:, lanes:] = out_im.astype(jnp.bfloat16)


def filtered_cross(fibre_got, band_got, segment_keep, band_mask):
    width = fibre_got.shape[0]
    cosines, sines = wave_tables(width)
    return pl.pallas_call(
        cross_kernel,
        out_shape=jax.ShapeDtypeStruct((width, 2 * SEG), jnp.bfloat16),
        compiler_params=pltpu.CompilerParams(vmem_limit_bytes=12 << 20),
        name="filtered_cross",
    )(fibre_got, band_got, segment_keep.reshape(1, SEG), band_mask, cosines, sines)


def place_kernel(got_ref, out_ref):
    rows = got_ref.shape[0] // NPART
    for q in range(NPART):
        for p in range(2):
            part = got_ref[q * rows : (q + 1) * rows, p * SEG : (p + 1) * SEG].astype(jnp.float32)
            out_ref[p, :, :, q * SEG : (q + 1) * SEG] = part.reshape(NFREQ, rows // NFREQ, SEG)


def place_out(got, here):
    return pl.pallas_call(
        place_kernel,
        out_shape=jax.ShapeDtypeStruct((2, NFREQ, here, NPART * SEG), jnp.float32),
        compiler_params=pltpu.CompilerParams(vmem_limit_bytes=12 << 20),
        name="place_out",
    )(got)


def exchange(rows, count, groups=None):
    lanes = rows.shape[1]
    blocks = rows.reshape(count, rows.shape[0] // count, lanes)
    blocks = lax.all_to_all(
        blocks, "chan", split_axis=0, concat_axis=0, tiled=True, axis_index_groups=groups
    )
    return blocks.reshape(rows.shape)


def shards(fibre_records, station_records, band_mask, station_valid, segment_keep):
    count = lax.axis_size("chan")
    here, stations = fibre_records.shape[0], station_records.shape[0]
    quarters = [[q * NFREQ + b for b in range(NFREQ)] for q in range(NPART)]
    fibre_send = spectra_call(fibre_kernel, fibre_records, (), count * here, here, 58)
    fibre_got = exchange(fibre_send, count)
    band_send = spectra_call(
        station_kernel, station_records, (station_valid,), NFREQ * stations, sum(STATION_CHUNKS), 58
    )
    band_got = exchange(band_send, NFREQ, quarters)
    back = filtered_cross(fibre_got, band_got, segment_keep, band_mask)
    return place_out(exchange(back, count), here)


def solution(mesh):
    placed = (P(("grp", "chan"), None, None), P("chan", None, None), P(), P("chan"), P())
    return jax.shard_map(
        shards,
        mesh=mesh,
        in_specs=placed,
        out_specs=P(None, None, ("grp", "chan"), None),
        check_vma=False,
    )
```
